32 devices in a mesh: src: 4 (over y, x), snk: 8 (over z, core).
Axes of the slice: x: 2, y: 2, z: 4, core: 2. Of those that a mesh axis runs over, the one named last changes fastest.
Arguments:
- perambulator: bfloat16 [4, 8, 2, 1024, 1024], P('src', 'snk'), may hold values from -0.25976562 to 0.25976562
- elementals: bfloat16 [8, 4, 2, 256, 256], P('snk', None, None, 'src'), may hold values from -0.25 to 0.25
- momentum: int32 [8], P('snk'), may hold values from 0 to 3
- routes: int32 [4, 8, 16, 1], P('src'), may hold values from 0 to 7; in each aligned block of 16 rows (0 to 15, 16 to 31, ..., all dimensions but the last counted through in order) at most 4 rows name the same one
- node_of: int32 [4, 8, 16], P('src'), may hold values from 0 to 7
- owner_slot: int32 [8], replicated, may hold values from 0 to 7, each once
Outputs:
- nodes: float32 [8, 2, 64, 1024], P('snk', None, 'src')
The draws below stay inside these ranges and needn't reach their ends.
Inputs may be any that keep to these rules, and one draw needn't show every extreme that they name: `routes`: among the 16 slabs of one tile (one s and k), at most 4 name the same sink timeslice. `owner_slot`: each value appears exactly once.
All inputs are finite; a program needn't handle non-finite values.
Results may differ from the reference program's by a relative error of at most 0.005.
Values may be sent and summed in bfloat16 or wider, within the bound.
No kernel may reach another device: no remote copies, remote signals or barrier semaphores. Data moves between devices by JAX's collectives and lax.ppermute only.
A program may use at most 128 MiB of HBM per device.

```python
import math
import jax
import jax.numpy as jnp
import numpy as np
from jax import lax

NEV = 256
SPIN = 4
M = 1024
NMOM = 4
RB = 64
NB = 16
CAP = 4
NNODE = 8
NS = 4
NK = 8


def place_ends(drawn, stream_key, least, largest):
    place = [jax.random.randint(jax.random.fold_in(stream_key, axis), (), 0, length) for axis, length in enumerate(drawn.shape)]
    main_axis = drawn.shape.index(max(drawn.shape))
    neighbour = place[:main_axis] + [(place[main_axis] + 1) % drawn.shape[main_axis]] + place[main_axis + 1:]
    return drawn.at[tuple(place)].set(least).at[tuple(neighbour)].set(largest)


def block_scale(rng, dims, pieces, low, largest):
    def one(dim, blocks):
        draws = jax.random.uniform(jax.random.fold_in(jax.random.fold_in(rng, 6), dim), (blocks,), jnp.float32, low / len(pieces), largest / len(pieces))
        return jnp.repeat(jnp.exp(draws), dims[dim] // blocks).reshape((-1,) + (1,) * (len(dims) - dim - 1))

    gain = one(*pieces[0])
    for cut in pieces[1:]:
        gain = gain * one(*cut)
    return gain


def deal_out(key, own, number, rows, count, top, bound, slope):
    ranking = jax.random.permutation(key, count)
    heavy_load, common = load_shares(count, rows * top, bound, slope, True), load_shares(count, rows * top, bound, slope, False)
    places = jnp.arange(count)

    def named(tallies, rotation):
        used = int((tallies > 0).sum())
        fixed = max(1, used // 4)
        moved = fixed + (places - fixed + rotation * (used - fixed)) % max(1, count - fixed)
        return jnp.zeros((count,), jnp.int32).at[ranking[jnp.where(places < fixed, places, moved)]].set(jnp.asarray(tallies, jnp.int32))

    tallies = jnp.where(number % 4 == 0, named(heavy_load, number // 4), named(common, number - number // 4 - 1))
    mixed = jax.random.permutation(jax.random.fold_in(own, 3), count)
    giver, receiver = mixed[0:count // 2 * 2:2], mixed[1:count // 2 * 2:2]
    margin = jnp.minimum(tallies[giver] - 1, bound - tallies[receiver]) // 2
    margin = jnp.where((giver == ranking[0]) | (receiver == ranking[0]) | (tallies[receiver] == 0), 0, jnp.maximum(margin, 0))
    moved = jax.random.randint(jax.random.fold_in(own, 4), (count // 2,), 0, 1 << 20) % (margin + 1)
    tallies = tallies.at[giver].add(-moved).at[receiver].add(moved)
    labels = jnp.searchsorted(jnp.cumsum(tallies), jnp.arange(rows * top), side="right").astype(jnp.int32)
    table = labels.reshape(top, rows).T
    table = table[jax.random.permutation(jax.random.fold_in(own, 1), rows)]
    rotation = jax.random.randint(jax.random.fold_in(own, 2), (rows, 1), 0, top)
    return jnp.take_along_axis(table, (jnp.arange(top)[None, :] + rotation) % top, axis=1)


def load_shares(number_of, total, bound, skew, full):
    portions = [(1 << 20) // math.isqrt(grade ** skew) + 1 for grade in range(1, number_of + 1)]
    largest = bound if full else min(bound, max(-(-total // number_of), total * portions[0] // sum(portions)))
    least = 1 if total - largest >= number_of - 1 else 0
    given, rest = [largest] + [least] * (number_of - 1), total - largest - least * (number_of - 1)
    while rest > 0:
        movable = [i for i in range(1, number_of) if given[i] < largest] or [i for i in range(1, number_of) if given[i] < bound]
        pool, left = sum([portions[i] for i in movable]), rest
        for i in movable:
            more = min(bound - given[i], max(1, left * portions[i] // pool), rest)
            given[i] = given[i] + more
            rest = rest - more
    return np.array(given)


def normal_values(stream_key, dims, spread, reach, pieces=(), held_as=jnp.bfloat16):
    array = jax.random.normal(stream_key, dims, jnp.float32) * spread
    if len(pieces) > 0:
        array = block_scale(stream_key, dims, pieces, -0.22, 0.18) * array
    return jnp.clip(array, min=-reach, max=reach).astype(held_as)


def setup_inputs(seed: int = 0) -> dict:
    key_of = jax.random.split(jax.random.key(seed), 7)
    perambulator = normal_values(key_of[0], (NS, NK, 2, M, M), 0.044, 0.25976562, ((0, 4), (1, 8)))
    elementals = normal_values(key_of[1], (NK, NMOM, 2, NEV, NEV), (2 * NEV) ** -0.5, 0.25, ((0, 8), (3, 4)))
    momentum = place_ends(jax.random.randint(key_of[2], (NK,), 0, NMOM), jax.random.fold_in(key_of[2], 1), 0, NMOM - 1).astype(jnp.int32)
    routes_keys = jax.random.split(jax.random.fold_in(key_of[3], 1), NS * NK * NB // NB)
    routes_turns = jax.random.permutation(jax.random.fold_in(key_of[3], 3), NS * NK * NB // NB)
    routes = jax.vmap(lambda own, number: deal_out(jax.random.fold_in(key_of[3], 2), own, number, NB, NK, 1, CAP, 2))(routes_keys, routes_turns).reshape((NS, NK, NB, 1))
    node_of = place_ends(jax.random.randint(key_of[4], (NS, NK, NB), 0, NNODE), jax.random.fold_in(key_of[4], 1), 0, NNODE - 1).astype(jnp.int32)
    owner_slot = jax.random.permutation(key_of[5], NNODE).astype(jnp.int32)
    return dict(perambulator=perambulator, elementals=elementals, momentum=momentum, routes=routes, node_of=node_of, owner_slot=owner_slot)


def dress(phi, source_tile):
    right = source_tile.reshape(2, NEV, SPIN * M)
    real_part = jnp.dot(phi[0], right[0], preferred_element_type=jnp.float32) - jnp.dot(phi[1], right[1], preferred_element_type=jnp.float32)
    imag_part = jnp.dot(phi[0], right[1], preferred_element_type=jnp.float32) + jnp.dot(phi[1], right[0], preferred_element_type=jnp.float32)
    return jnp.stack([real_part, imag_part]).astype(jnp.bfloat16).reshape(2, M, M)


def times_adjoint(slab_rows, partner):
    real_part = jnp.dot(slab_rows[0], partner[0].T, preferred_element_type=jnp.float32) + jnp.dot(slab_rows[1], partner[1].T, preferred_element_type=jnp.float32)
    imag_part = jnp.dot(slab_rows[1], partner[0].T, preferred_element_type=jnp.float32) - jnp.dot(slab_rows[0], partner[1].T, preferred_element_type=jnp.float32)
    return jnp.stack([real_part, imag_part])


def reference(perambulator, elementals, momentum, routes, node_of, owner_slot):
    sinks = jnp.arange(NK, dtype=jnp.int32)
    phis = elementals[sinks, momentum.astype(jnp.int32)]

    def per_source(source, totals):
        tiles = perambulator[source]
        dressed = lax.map(lambda pair: dress(pair[0], pair[1]), (phis, tiles))
        slabs = dressed.reshape(NK, 2, NB, RB, M)

        def per_slab(index, inner):
            sink = (index // NB).astype(jnp.int32)
            block = (index % NB).astype(jnp.int32)
            chosen = slabs[sink][:, block]
            helper = routes[source, sink, block, 0].astype(jnp.int32)
            partner = dressed[helper]
            product = times_adjoint(chosen, partner)
            position = owner_slot[node_of[source, sink, block]].astype(jnp.int32)
            return inner.at[position].add(product)

        return lax.fori_loop(0, NK * NB, per_slab, totals)

    start = jnp.zeros((NNODE, 2, RB, M), jnp.float32)
    return lax.fori_loop(0, NS, per_source, start)
```

```python
import functools

import jax
import jax.numpy as jnp
from jax import lax
from jax.experimental import pallas as pl
from jax.experimental.pallas import tpu as pltpu
from jax.sharding import PartitionSpec as P

F32 = jnp.float32
BF16 = jnp.bfloat16
VMEM = pl.BlockSpec(memory_space=pltpu.VMEM)
SMEM = pl.BlockSpec(memory_space=pltpu.SMEM)
ANY = pl.BlockSpec(memory_space=pl.ANY)


def params(mib):
    return pltpu.CompilerParams(vmem_limit_bytes=mib * 1024 * 1024)


def swap(value, axis, size, flip):
    return lax.ppermute(value, axis, [(i, i ^ flip) for i in range(size)])


def cut_kernel(where_ref, tile_ref, out_ref):
    out_ref[...] = tile_ref[...]


def cut(tile, where, width):
    _, order, _ = tile.shape
    steps = 4
    rows = order // steps
    return pl.pallas_call(
        cut_kernel,
        out_shape=jax.ShapeDtypeStruct((2, order, width), tile.dtype),
        grid_spec=pltpu.PrefetchScalarGridSpec(
            num_scalar_prefetch=1,
            grid=(steps,),
            in_specs=[pl.BlockSpec((2, rows, width), lambda i, where: (0, i, where[0]))],
            out_specs=pl.BlockSpec((2, rows, width), lambda i, where: (0, i, 0)),
        ),
        compiler_params=params(16),
        cost_estimate=pl.CostEstimate(
            flops=0, bytes_accessed=8 * order * width, transcendentals=0
        ),
        name="cut",
    )(where, tile)


def widen_kernel(spin, phi_ref, out_ref):
    eigen = phi_ref.shape[-1]
    order = eigen * spin
    row = lax.broadcasted_iota(jnp.int32, (order, eigen), 0)
    col = lax.broadcasted_iota(jnp.int32, (order, eigen), 1)
    spread = (row // spin == col).astype(BF16)
    rows = eigen
    for x in range(2):
        tall = jnp.dot(spread, phi_ref[x], preferred_element_type=F32).astype(BF16)
        for part in range(order // rows):
            piece = tall[part * rows : (part + 1) * rows]
            wide = lax.dot_general(
                piece, spread, (((1,), (1,)), ((), ())), preferred_element_type=F32
            )
            r = lax.broadcasted_iota(jnp.int32, (rows, order), 0)
            c = lax.broadcasted_iota(jnp.int32, (rows, order), 1)
            same = (r + part * rows) % spin == c % spin
            out_ref[x, part * rows : (part + 1) * rows, :] = jnp.where(same, wide, 0.0).astype(
                BF16
            )


def widen(phi, spin):
    eigen = phi.shape[-1]
    order = eigen * spin
    return pl.pallas_call(
        functools.partial(widen_kernel, spin),
        out_shape=jax.ShapeDtypeStruct((2, order, order), BF16),
        in_specs=[VMEM],
        out_specs=VMEM,
        compiler_params=params(32),
        cost_estimate=pl.CostEstimate(
            flops=4 * order * eigen * (eigen + order), bytes_accessed=4 * order * order, transcendentals=0
        ),
        name="widen",
    )(phi)


def dress_kernel(where_ref, wide_ref, tile_ref, out_ref):
    k0, k1 = wide_ref[0], wide_ref[1]
    p0, p1 = tile_ref[0], tile_ref[1]
    dot = functools.partial(jnp.dot, preferred_element_type=F32)
    out_ref[0] = (dot(k0, p0) - dot(k1, p1)).astype(BF16)
    out_ref[1] = (dot(k0, p1) + dot(k1, p0)).astype(BF16)


def dress(wide, tile, where, width):
    _, order, _ = tile.shape
    steps = 4
    rows = order // steps
    return pl.pallas_call(
        dress_kernel,
        out_shape=jax.ShapeDtypeStruct((2, order, width), BF16),
        grid_spec=pltpu.PrefetchScalarGridSpec(
            num_scalar_prefetch=1,
            grid=(steps,),
            in_specs=[
                pl.BlockSpec((2, rows, order), lambda i, where: (0, i, 0)),
                pl.BlockSpec((2, order, width), lambda i, where: (0, 0, where[0])),
            ],
            out_specs=pl.BlockSpec((2, rows, width), lambda i, where: (0, i, 0)),
        ),
        compiler_params=params(32),
        cost_estimate=pl.CostEstimate(
            flops=8 * order * order * width,
            bytes_accessed=4 * order * (order + 2 * width),
            transcendentals=0,
        ),
        name="dress",
    )(where, wide, tile)


def add_slabs(dest_ref, sink, tile_ref, sums_ref):
    slab_count = dest_ref.shape[1]
    slab_rows = tile_ref.shape[1] // slab_count

    def one(b, carry):
        dest = dest_ref[sink, b]

        @pl.when(dest >= 0)
        def _():
            start = pl.multiple_of(b * slab_rows, slab_rows)
            sums_ref[dest] += tile_ref[:, pl.ds(start, slab_rows), :].astype(F32)

        return carry

    lax.fori_loop(0, slab_count, one, 0)


def gather_kernel(count, sinks_ref, dest_ref, *refs):
    tiles, sums_ref = refs[:count], refs[count]

    def clear(i, carry):
        sums_ref[i] = jnp.zeros(sums_ref.shape[1:], F32)
        return carry

    lax.fori_loop(0, sums_ref.shape[0], clear, 0)
    for i, tile_ref in enumerate(tiles):
        add_slabs(dest_ref, sinks_ref[i], tile_ref, sums_ref)


def gather(sinks, dest, tiles, groups):
    _, order, width = tiles[0].shape
    slab_rows = order // dest.shape[1]
    return pl.pallas_call(
        functools.partial(gather_kernel, len(tiles)),
        out_shape=jax.ShapeDtypeStruct((groups, 2, slab_rows, width), F32),
        in_specs=[SMEM, SMEM] + [VMEM] * len(tiles),
        out_specs=VMEM,
        compiler_params=params(48),
        cost_estimate=pl.CostEstimate(
            flops=4 * len(tiles) * order * width,
            bytes_accessed=4 * len(tiles) * order * width + 8 * groups * slab_rows * width,
            transcendentals=0,
        ),
        name="gather",
    )(sinks, dest, *tiles)


def finish_kernel(
    count, late, nodes, parts, sinks_ref, dest_ref, here_ref, sums_hbm, *refs
):
    tiles = refs[:count]
    outs = refs[count : count + parts]
    tile_ref, late_ref, sums_ref, left_ref, total_ref, sems = refs[count + parts :]
    _, order, width = tiles[0].shape
    slab_rows = sums_ref.shape[2]

    late_copies = [
        pltpu.make_async_copy(tiles[count - late + i], late_ref.at[i], sems.at[i])
        for i in range(late)
    ]
    sums_copy = pltpu.make_async_copy(sums_hbm, sums_ref, sems.at[late])
    tile_copies = []
    for i in range(count):
        for x in range(2):
            span = pl.ds((2 * i + x) * width, width)
            tile_copies.append(
                pltpu.make_async_copy(
                    tiles[i].at[x], tile_ref.at[:, span], sems.at[late + 1 + 2 * i + x]
                )
            )
    for copy in late_copies:
        copy.start()
    sums_copy.start()
    for copy in tile_copies:
        copy.start()
    for copy in late_copies:
        copy.wait()
    sums_copy.wait()
    for i in range(late):
        add_slabs(dest_ref, sinks_ref[count - late + i], late_ref.at[i], sums_ref)

    def place(node, carry):
        rows = pl.multiple_of(node * 2 * slab_rows, 2 * slab_rows)
        for i in range(count):
            real = sums_ref[i * nodes + node, 0].astype(BF16)
            imag = sums_ref[i * nodes + node, 1].astype(BF16)
            first = slice(2 * i * width, (2 * i + 1) * width)
            second = slice((2 * i + 1) * width, (2 * i + 2) * width)
            left_ref[pl.ds(rows, slab_rows), first] = real
            left_ref[pl.ds(rows + slab_rows, slab_rows), first] = imag
            left_ref[pl.ds(rows, slab_rows), second] = imag
            left_ref[pl.ds(rows + slab_rows, slab_rows), second] = -real
        return carry

    lax.fori_loop(0, nodes, place, 0)
    for copy in tile_copies:
        copy.wait()
    block = 256

    def multiply(j, carry):
        cols = pl.multiple_of(j * block, block)
        product = lax.dot_general(
            left_ref[...],
            tile_ref[pl.ds(cols, block), :],
            (((1,), (1,)), ((), ())),
            preferred_element_type=F32,
        )
        total_ref[:, :, pl.ds(cols, block)] = product.reshape(2 * nodes, slab_rows, block)
        return carry

    lax.fori_loop(0, order // block, multiply, 0)
    rows = slab_rows // parts
    for u in range(parts):
        start = pl.multiple_of((here_ref[0] ^ u) * rows, rows)
        outs[u][...] = total_ref[:, pl.ds(start, rows), :].astype(outs[u].dtype)


def finish(sinks, dest, here, sums, tiles, late, nodes, parts):
    _, order, width = tiles[0].shape
    count = len(tiles)
    slab_rows = sums.shape[2]
    shape = (2 * nodes, slab_rows // parts, order)
    return pl.pallas_call(
        functools.partial(finish_kernel, count, late, nodes, parts),
        out_shape=[jax.ShapeDtypeStruct(shape, BF16 if u else F32) for u in range(parts)],
        in_specs=[SMEM, SMEM, SMEM] + [ANY] * (count + 1),
        out_specs=[VMEM] * parts,
        scratch_shapes=[
            pltpu.VMEM((order, 2 * count * width), BF16),
            pltpu.VMEM((late, 2, order, width), BF16),
            pltpu.VMEM(sums.shape, F32),
            pltpu.VMEM((2 * nodes * slab_rows, 2 * count * width), BF16),
            pltpu.VMEM((2 * nodes, slab_rows, order), F32),
            pltpu.SemaphoreType.DMA((late + 1 + 2 * count,)),
        ],
        compiler_params=params(56),
        cost_estimate=pl.CostEstimate(
            flops=8 * nodes * slab_rows * order * count * width,
            bytes_accessed=4 * count * order * width + 4 * sums.size,
            transcendentals=0,
        ),
        name="finish",
    )(sinks, dest, here, sums, *tiles)


def on_device(perambulator, elementals, momentum, routes, node_of, owner_slot):
    tile = perambulator[0, 0]
    order = tile.shape[1]
    eigen = elementals.shape[-1]
    spin = order // eigen
    sink_count = lax.axis_size("snk")
    source_count = lax.axis_size("src")
    chips = sink_count // 2
    width = order // chips
    node_count = owner_slot.shape[0]
    nodes = node_count // 2
    sink = lax.axis_index("snk")
    source = lax.axis_index("src")
    chip, core = sink // 2, sink % 2
    raw = chips // 2
    steps = [t for t in range(1, chips) if t != raw]
    sends = lambda value, t: swap(value, "snk", sink_count, 2 * t)
    column = lambda t: (chip ^ t).astype(jnp.int32).reshape(1)

    route = routes[0, :, :, 0]
    node_ids = jnp.arange(node_count, dtype=jnp.int32)
    match = (node_of[0][:, :, None] == node_ids).astype(jnp.int32)
    position = jnp.sum(match * owner_slot, axis=2)
    partner = 2 * ((route // 2) ^ chip) + ((route % 2) ^ core)

    piece = lax.dynamic_index_in_dim(elementals[0], momentum[0], 0, False)
    far_piece = sends(piece, raw)
    far_raw = sends(cut(tile, column(raw), width), raw)
    phis = lax.all_gather(jnp.stack([piece, far_piece]), "src", axis=2, tiled=True)
    wide = widen(phis[0], spin)
    dressed = {t: sends(dress(wide, tile, column(t), width), t) for t in steps}
    dressed[0] = dress(wide, tile, column(0), width)
    far_wide = widen(phis[1], spin)
    dressed[raw] = dress(far_wide, far_raw, jnp.zeros((1,), jnp.int32), width)

    arrival = [0, raw] + steps
    tiles = []
    sinks = []
    places = []
    for t in arrival:
        tiles += [dressed[t], swap(dressed[t], "snk", sink_count, 1)]
        sinks += [2 * (chip ^ t) + core, 2 * (chip ^ t) + (1 - core)]
        places += [2 * t, 2 * t + 1]
    sinks = jnp.stack(sinks).astype(jnp.int32)
    rank = [places.index(i) for i in range(sink_count)]
    ids = jnp.arange(sink_count, dtype=jnp.int32)
    order_of = jnp.sum(
        (partner[:, :, None] == ids).astype(jnp.int32) * jnp.array(rank, jnp.int32), axis=2
    )
    dest = jnp.where(position % 2 == core, order_of * nodes + position // 2, -1).astype(jnp.int32)
    late = 2
    early = len(tiles) - late
    sums = gather(sinks[:early], dest, tiles[:early], sink_count * nodes)
    here = source.astype(jnp.int32).reshape(1)
    outs = finish(sinks, dest, here, sums, tiles, late, nodes, source_count)

    moved = [outs[0]]
    for u in list(range(1, source_count))[::-1]:
        moved.append(swap(outs[u], "src", source_count, u).astype(F32))
    total = functools.reduce(jnp.add, moved)
    total = total.reshape((nodes, 2) + total.shape[1:])
    pick = lambda t: lax.dynamic_index_in_dim(total, chip ^ t, 0, True)
    result = pick(0)
    for t in list(range(1, chips))[::-1]:
        result = result + sends(pick(t).astype(BF16), t).astype(F32)
    return result


def solution(mesh):
    placed = (
        P("src", "snk", None, None, None),
        P("snk", None, None, "src", None),
        P("snk"),
        P("src", None, None, None),
        P("src", None, None),
        P(),
    )
    return jax.shard_map(
        on_device,
        mesh=mesh,
        in_specs=placed,
        out_specs=P("snk", None, "src", None),
        check_vma=False,
    )
```

```python
import functools

import jax
import jax.numpy as jnp
from jax import lax
from jax.experimental import pallas as pl
from jax.experimental.pallas import tpu as pltpu
from jax.sharding import PartitionSpec as P


FINISH_MIB = 40
F32 = jnp.float32
BF16 = jnp.bfloat16
VMEM = pl.BlockSpec(memory_space=pltpu.VMEM)
SMEM = pl.BlockSpec(memory_space=pltpu.SMEM)
ANY = pl.BlockSpec(memory_space=pl.ANY)


def params(mib):
    return pltpu.CompilerParams(vmem_limit_bytes=mib * 1024 * 1024)


def swap(value, axis, size, flip):
    return lax.ppermute(value, axis, [(i, i ^ flip) for i in range(size)])


def cut_kernel(where_ref, tile_hbm, out_ref, sems):
    width = out_ref.shape[-1] // 2
    start = pl.multiple_of(where_ref[0] * width, width)
    copies = [
        pltpu.make_async_copy(
            tile_hbm.at[x, :, pl.ds(start, width)],
            out_ref.at[:, x * width : (x + 1) * width],
            sems.at[x],
        )
        for x in range(2)
    ]
    for copy in copies:
        copy.start()
    for copy in copies:
        copy.wait()


def cut(tile, where, width):
    _, order, _ = tile.shape
    return pl.pallas_call(
        cut_kernel,
        out_shape=jax.ShapeDtypeStruct((order, 2 * width), tile.dtype),
        in_specs=[SMEM, ANY],
        out_specs=VMEM,
        scratch_shapes=[pltpu.SemaphoreType.DMA((2,))],
        compiler_params=params(60),
        cost_estimate=pl.CostEstimate(
            flops=0, bytes_accessed=8 * order * width, transcendentals=0
        ),
        name="cut",
    )(where, tile)


def dress_kernel(spin, pieces, where_ref, phi_ref, tile_ref, *refs):
    refs = list(refs)
    outs = [[refs.pop(0) for _ in range(n)] for n in pieces]
    sems = refs.pop()
    wide_ref = refs.pop()
    rights = refs
    order = wide_ref.shape[0]
    eigen = order // spin
    copies = []
    for j, right_ref in enumerate(rights):
        width = right_ref.shape[1] // 2
        for x in range(2):
            if len(tile_ref.shape) == 3:
                start = pl.multiple_of(where_ref[j] * width, width)
                source = tile_ref.at[x, :, pl.ds(start, width)]
            else:
                source = tile_ref.at[:, x * width : (x + 1) * width]
            target = right_ref.at[:order, x * width : (x + 1) * width]
            copies.append(pltpu.make_async_copy(source, target, sems.at[2 * j + x]))
            copies[-1].start()

    row = lax.broadcasted_iota(jnp.int32, (order, eigen), 0)
    col = lax.broadcasted_iota(jnp.int32, (order, eigen), 1)
    spread = (row // spin == col).astype(BF16)
    r = lax.broadcasted_iota(jnp.int32, (eigen, order), 0)
    c = lax.broadcasted_iota(jnp.int32, (eigen, order), 1)
    same = r % spin == c % spin
    for x in range(2):
        tall = jnp.dot(spread, phi_ref[x], preferred_element_type=F32).astype(BF16)
        for part in range(spin):
            rows = slice(part * eigen, (part + 1) * eigen)
            wide = lax.dot_general(
                tall[rows], spread, (((1,), (1,)), ((), ())), preferred_element_type=F32
            )
            wide_ref[rows, x * order : (x + 1) * order] = jnp.where(same, wide, 0.0).astype(BF16)

    block = 256
    for j, right_ref in enumerate(rights):
        copies[2 * j].wait()
        copies[2 * j + 1].wait()
        width = right_ref.shape[1] // 2
        right_ref[order:, :width] = -right_ref[:order, width:]
        right_ref[order:, width:] = right_ref[:order, :width]

        def multiply(i, carry):
            rows = pl.ds(pl.multiple_of(i * block, block), block)
            both = jnp.dot(
                wide_ref[rows, :], right_ref[...], preferred_element_type=F32
            ).astype(BF16)
            part = width // len(outs[j])
            for k, out_ref in enumerate(outs[j]):
                out_ref[rows, :part] = both[:, k * part : (k + 1) * part]
                out_ref[rows, part:] = both[:, width + k * part : width + (k + 1) * part]
            return carry

        lax.fori_loop(0, order // block, multiply, 0)


def dress(phi, spin, tile, where, widths, pieces):
    order = phi.shape[-1] * spin
    outs = []
    for width, n in zip(widths, pieces):
        outs += [jax.ShapeDtypeStruct((order, 2 * width // n), BF16)] * n
    scratch = [pltpu.VMEM((2 * order, 2 * width), BF16) for width in widths]
    scratch += [
        pltpu.VMEM((order, 2 * order), BF16),
        pltpu.SemaphoreType.DMA((2 * len(widths),)),
    ]
    flat = pl.pallas_call(
        functools.partial(dress_kernel, spin, pieces),
        out_shape=outs,
        in_specs=[SMEM, VMEM, ANY],
        out_specs=[VMEM] * len(outs),
        scratch_shapes=scratch,
        compiler_params=params(58),
        cost_estimate=pl.CostEstimate(
            flops=8 * order * order * sum(widths),
            bytes_accessed=8 * order * sum(widths),
            transcendentals=0,
        ),
        name="dress",
    )(where, phi, tile)
    flat = list(flat)
    return [[flat.pop(0) for _ in range(n)] for n in pieces]


def clear(sums_ref):
    def one(i, carry):
        sums_ref[i] = jnp.zeros(sums_ref.shape[1:], F32)
        return carry

    lax.fori_loop(0, sums_ref.shape[0], one, 0)


def add_slabs(dest_ref, sink, tile_ref, sums_ref, base=0):
    groups, slab_rows, _ = sums_ref.shape

    def one(b, carry):
        dest = dest_ref[sink, b] - base

        @pl.when(jnp.logical_and(dest >= 0, dest < groups))
        def _():
            start = pl.multiple_of(b * slab_rows, slab_rows)
            sums_ref[dest] += tile_ref[pl.ds(start, slab_rows), :].astype(F32)

        return carry

    lax.fori_loop(0, tile_ref.shape[0] // slab_rows, one, 0)


def gather_kernel(count, sinks_ref, dest_ref, *refs):
    sums_ref = refs[count]
    clear(sums_ref)
    for i, tile_ref in enumerate(refs[:count]):
        add_slabs(dest_ref, sinks_ref[i], tile_ref, sums_ref)


def gather(sinks, dest, tiles, groups):
    order, width = tiles[0].shape
    slab_rows = order // dest.shape[1]
    return pl.pallas_call(
        functools.partial(gather_kernel, len(tiles)),
        out_shape=jax.ShapeDtypeStruct((groups, slab_rows, width), F32),
        in_specs=[SMEM, SMEM] + [VMEM] * len(tiles),
        out_specs=VMEM,
        compiler_params=params(24),
        cost_estimate=pl.CostEstimate(
            flops=len(tiles) * order * width,
            bytes_accessed=2 * len(tiles) * order * width + 4 * groups * slab_rows * width,
            transcendentals=0,
        ),
        name="gather",
    )(sinks, dest, *tiles)


def finish_kernel(count, late, nodes, base, first, last, sinks_ref, dest_ref, here_ref, *refs):
    refs = list(refs)
    early_ref = None if late == count else refs.pop(0)
    before_ref = None if first else refs.pop(0)
    tiles = [refs.pop(0) for _ in range(count)]
    total_ref = refs.pop() if last else refs[0]
    left_ref = refs.pop()
    sums_ref = refs.pop()
    outs = refs
    order, width = tiles[0].shape
    half = width // 2
    slab_rows = sums_ref.shape[1]

    groups = sums_ref.shape[0]
    start = base * count
    if early_ref is None:
        clear(sums_ref)
    else:

        def take(i, carry):
            sums_ref[i] = early_ref[start + i]
            return carry

        lax.fori_loop(0, groups, take, 0)
    for i in range(count - late, count):
        add_slabs(dest_ref, sinks_ref[i], tiles[i], sums_ref, start)

    def place(node, carry):
        rows = pl.multiple_of(node * 2 * slab_rows, 2 * slab_rows)
        for i in range(count):
            real = sums_ref[node * count + i, :, :half].astype(BF16)
            imag = sums_ref[node * count + i, :, half:].astype(BF16)
            one = slice(i * width, i * width + half)
            two = slice(i * width + half, (i + 1) * width)
            left_ref[pl.ds(rows, slab_rows), one] = real
            left_ref[pl.ds(rows + slab_rows, slab_rows), one] = imag
            left_ref[pl.ds(rows, slab_rows), two] = imag
            left_ref[pl.ds(rows + slab_rows, slab_rows), two] = -real
        return carry

    lax.fori_loop(0, nodes, place, 0)
    block = 256

    def multiply(j, carry):
        cols = pl.ds(pl.multiple_of(j * block, block), block)
        rows = pl.ds(2 * base, 2 * nodes)
        product = 0.0 if first else before_ref[rows, :, cols].reshape(-1, block)
        for i in range(count):
            product += lax.dot_general(
                left_ref[:, i * width : (i + 1) * width],
                tiles[i][cols, :],
                (((1,), (1,)), ((), ())),
                preferred_element_type=F32,
            )
        total_ref[:, :, cols] = product.reshape(2 * nodes, slab_rows, block)
        return carry

    lax.fori_loop(0, order // block, multiply, 0)
    if last:
        rows = slab_rows // len(outs)
        for u, out_ref in enumerate(outs):
            start = pl.multiple_of((here_ref[0] ^ u) * rows, rows)
            out_ref[...] = total_ref[:, pl.ds(start, rows), :].astype(out_ref.dtype)


def finish(sinks, dest, here, sums, before, tiles, late, nodes, base, parts):
    order, width = tiles[0].shape
    count = len(tiles)
    slab_rows = order // dest.shape[1]
    first, last = before is None, parts > 0
    whole = jax.ShapeDtypeStruct((2 * nodes, slab_rows, order), F32)
    shape = (2 * nodes, slab_rows // max(parts, 1), order)
    outs = [jax.ShapeDtypeStruct(shape, BF16 if u else F32) for u in range(parts)]
    extra = [a for a in (sums, before) if a is not None]
    scratch = [
        pltpu.VMEM((count * nodes, slab_rows, width), F32),
        pltpu.VMEM((2 * nodes * slab_rows, count * width), BF16),
    ]
    if last:
        scratch.append(pltpu.VMEM(whole.shape, F32))
    return pl.pallas_call(
        functools.partial(finish_kernel, count, late, nodes, base, first, last),
        out_shape=outs if last else [whole],
        in_specs=[SMEM, SMEM, SMEM] + [VMEM] * (count + len(extra)),
        out_specs=[VMEM] * max(parts, 1),
        scratch_shapes=scratch,
        compiler_params=params(FINISH_MIB),
        cost_estimate=pl.CostEstimate(
            flops=8 * nodes * slab_rows * order * count * width,
            bytes_accessed=2 * count * order * width,
            transcendentals=0,
        ),
        name="finish",
    )(sinks, dest, here, *extra, *tiles)


def on_device(perambulator, elementals, momentum, routes, node_of, owner_slot):
    tile = perambulator[0, 0]
    order = tile.shape[1]
    eigen = elementals.shape[-1]
    spin = order // eigen
    sink_count = lax.axis_size("snk")
    source_count = lax.axis_size("src")
    chips = sink_count // 2
    width = order // chips
    node_count = owner_slot.shape[0]
    nodes = node_count // 2
    sink = lax.axis_index("snk")
    source = lax.axis_index("src")
    chip, core = sink // 2, sink % 2
    raw = chips // 2
    steps = [t for t in range(1, chips) if t != raw]
    sends = lambda value, t: swap(value, "snk", sink_count, 2 * t)
    column = lambda t: (chip ^ t).astype(jnp.int32).reshape(1)

    route = routes[0, :, :, 0]
    node_ids = jnp.arange(node_count, dtype=jnp.int32)
    match = (node_of[0][:, :, None] == node_ids).astype(jnp.int32)
    position = jnp.sum(match * owner_slot, axis=2)
    partner = 2 * ((route // 2) ^ chip) + ((route % 2) ^ core)

    chunks = 2 if width % 256 == 0 else 1
    part = width // chunks
    tie = lax.optimization_barrier

    first = cut(tile, column(raw) * chunks, part)
    far_raw = sends(first, raw)
    piece = lax.dynamic_index_in_dim(elementals[0], momentum[0], 0, False)
    piece, first = tie((piece, first))
    phi = near_phi = lax.all_gather(piece, "src", axis=1, tiled=True)
    own = {}
    (own[steps[-1]],) = dress(phi, spin, tile, column(steps[-1]), [width], [chunks])
    phi, own[steps[-1]] = tie((phi, own[steps[-1]]))
    rest = ([raw] if chunks > 1 else []) + steps[-2::-1] + [0]
    where = [column(t) * chunks + 1 if t == raw else column(t) for t in rest]
    made = dress(
        phi,
        spin,
        tile,
        jnp.concatenate(where),
        [part if t == raw else width for t in rest],
        [1 if t == raw else chunks for t in rest],
    )
    own.update(zip(rest, made))
    if chunks > 1:
        own[raw] = [None] + own[raw]
    piece, near_phi = tie((piece, near_phi))
    far_piece = sends(piece, raw)
    far_phi = lax.all_gather(far_piece, "src", axis=1, tiled=True)

    here = source.astype(jnp.int32).reshape(1)
    arrival = [0, raw] + steps
    sinks = []
    places = []
    for t in arrival:
        sinks += [2 * (chip ^ t) + core, 2 * (chip ^ t) + (1 - core)]
        places += [2 * t, 2 * t + 1]
    sinks = jnp.stack(sinks).astype(jnp.int32)
    rank = jnp.array([places.index(i) for i in range(sink_count)], jnp.int32)
    ids = jnp.arange(sink_count, dtype=jnp.int32)
    order_of = jnp.sum((partner[:, :, None] == ids).astype(jnp.int32) * rank, axis=2)
    slot = ((position // 2) ^ chip) * sink_count + order_of
    dest = jnp.where(position % 2 == core, slot, -1).astype(jnp.int32)

    total = None
    seen = {}
    for c in range(chunks):
        here_now = {0: own[0][c]}
        if c:
            for t in [raw] + steps:
                sent, _ = tie((own[t][c], seen[t]))
                here_now[t] = sends(sent, t)
        else:
            for t in steps[::-1]:
                here_now[t] = seen[t] = sends(own[t][c], t)
            seen[raw] = far_raw
            for t in steps[:-1]:
                seen[t] = own[t][0]
            zero = jnp.zeros((1,), jnp.int32)
            (here_now[raw],) = dress(far_phi, spin, far_raw, zero, [part], [1])[0]
        tiles = []
        for t in arrival:
            tiles += [here_now[t], swap(here_now[t], "snk", sink_count, 1)]
        count = len(tiles)
        if c < chunks - 1:
            (total,) = finish(sinks, dest, here, None, total, tiles, count, nodes, 0, 0)
        else:
            late = 2
            sums = gather(sinks, dest, tiles[: count - late], sink_count * nodes)

    half = nodes // 2
    kept = []
    for base in (half, 0):
        outs = finish(sinks, dest, here, sums, total, tiles, late, half, base, source_count)
        moved = [outs[0]]
        for u in list(range(1, source_count))[::-1]:
            moved.append(swap(outs[u], "src", source_count, u).astype(F32))
        summed = functools.reduce(jnp.add, moved)
        summed = summed.reshape((half, 2) + summed.shape[1:])
        for t in list(range(base, base + half))[::-1]:
            value = summed[t - base]
            kept.append(sends(value.astype(BF16), t).astype(F32) if t else value)
    return functools.reduce(jnp.add, kept[::-1])[None]


def solution(mesh):
    placed = (
        P("src", "snk", None, None, None),
        P("snk", None, None, "src", None),
        P("snk"),
        P("src", None, None, None),
        P("src", None, None),
        P(),
    )
    return jax.shard_map(
        on_device,
        mesh=mesh,
        in_specs=placed,
        out_specs=P("snk", None, "src", None),
        check_vma=False,
    )
```

```python
import functools

import jax
import jax.numpy as jnp
from jax import lax
from jax.experimental import pallas as pl
from jax.experimental.pallas import tpu as pltpu
from jax.sharding import PartitionSpec as P


FINISH_MIB = 40
F32 = jnp.float32
BF16 = jnp.bfloat16
VMEM = pl.BlockSpec(memory_space=pltpu.VMEM)
SMEM = pl.BlockSpec(memory_space=pltpu.SMEM)
ANY = pl.BlockSpec(memory_space=pl.ANY)


def params(mib):
    return pltpu.CompilerParams(vmem_limit_bytes=mib * 1024 * 1024)


def swap(value, axis, size, flip):
    return lax.ppermute(value, axis, [(i, i ^ flip) for i in range(size)])


def cut_kernel(steps, where_ref, tile_hbm, out_hbm, held_ref, in_sems, out_sems):
    order, width = held_ref.shape
    half = width // 2
    start = pl.multiple_of(where_ref[0] * half, half)
    rows = order // steps
    into, out = [], []
    for i in range(steps):
        span = slice(i * rows, (i + 1) * rows)
        for x in range(2):
            held = held_ref.at[span, x * half : (x + 1) * half]
            into.append(
                pltpu.make_async_copy(
                    tile_hbm.at[x, span, pl.ds(start, half)], held, in_sems.at[2 * i + x]
                )
            )
            out.append(
                pltpu.make_async_copy(
                    held, out_hbm.at[span, x * half : (x + 1) * half], out_sems.at[2 * i + x]
                )
            )
    for copy in into:
        copy.start()
    for copy, onward in zip(into, out):
        copy.wait()
        onward.start()
    for onward in out:
        onward.wait()


def cut(tile, where, width):
    _, order, _ = tile.shape
    steps = 4
    return pl.pallas_call(
        functools.partial(cut_kernel, steps),
        out_shape=jax.ShapeDtypeStruct((order, 2 * width), tile.dtype),
        in_specs=[SMEM, ANY],
        out_specs=ANY,
        scratch_shapes=[
            pltpu.VMEM((order, 2 * width), tile.dtype),
            pltpu.SemaphoreType.DMA((2 * steps,)),
            pltpu.SemaphoreType.DMA((2 * steps,)),
        ],
        compiler_params=params(60),
        cost_estimate=pl.CostEstimate(
            flops=0, bytes_accessed=8 * order * width, transcendentals=0
        ),
        name="cut",
    )(where, tile)


def dress_kernel(spin, pieces, where_ref, phi_ref, tile_ref, *refs):
    refs = list(refs)
    outs = [[refs.pop(0) for _ in range(n)] for n in pieces]
    sems = refs.pop()
    wide_ref = refs.pop()
    rights = refs
    order = wide_ref.shape[0]
    eigen = order // spin
    copies = []
    for j, right_ref in enumerate(rights):
        width = right_ref.shape[1] // 2
        for x in range(2):
            if len(tile_ref.shape) == 3:
                start = pl.multiple_of(where_ref[j] * width, width)
                source = tile_ref.at[x, :, pl.ds(start, width)]
            else:
                source = tile_ref.at[:, x * width : (x + 1) * width]
            target = right_ref.at[:order, x * width : (x + 1) * width]
            copies.append(pltpu.make_async_copy(source, target, sems.at[2 * j + x]))
            copies[-1].start()

    row = lax.broadcasted_iota(jnp.int32, (order, eigen), 0)
    col = lax.broadcasted_iota(jnp.int32, (order, eigen), 1)
    spread = (row // spin == col).astype(BF16)
    r = lax.broadcasted_iota(jnp.int32, (eigen, order), 0)
    c = lax.broadcasted_iota(jnp.int32, (eigen, order), 1)
    same = r % spin == c % spin
    for x in range(2):
        tall = jnp.dot(spread, phi_ref[x], preferred_element_type=F32).astype(BF16)
        for part in range(spin):
            rows = slice(part * eigen, (part + 1) * eigen)
            wide = lax.dot_general(
                tall[rows], spread, (((1,), (1,)), ((), ())), preferred_element_type=F32
            )
            wide_ref[rows, x * order : (x + 1) * order] = jnp.where(same, wide, 0.0).astype(BF16)

    block = 256
    for j, right_ref in enumerate(rights):
        copies[2 * j].wait()
        copies[2 * j + 1].wait()
        width = right_ref.shape[1] // 2
        right_ref[order:, :width] = -right_ref[:order, width:]
        right_ref[order:, width:] = right_ref[:order, :width]

        def multiply(i, carry):
            rows = pl.ds(pl.multiple_of(i * block, block), block)
            both = jnp.dot(
                wide_ref[rows, :], right_ref[...], preferred_element_type=F32
            ).astype(BF16)
            part = width // len(outs[j])
            for k, out_ref in enumerate(outs[j]):
                out_ref[rows, :part] = both[:, k * part : (k + 1) * part]
                out_ref[rows, part:] = both[:, width + k * part : width + (k + 1) * part]
            return carry

        lax.fori_loop(0, order // block, multiply, 0)


def dress(phi, spin, tile, where, widths, pieces):
    order = phi.shape[-1] * spin
    outs = []
    for width, n in zip(widths, pieces):
        outs += [jax.ShapeDtypeStruct((order, 2 * width // n), BF16)] * n
    scratch = [pltpu.VMEM((2 * order, 2 * width), BF16) for width in widths]
    scratch += [
        pltpu.VMEM((order, 2 * order), BF16),
        pltpu.SemaphoreType.DMA((2 * len(widths),)),
    ]
    flat = pl.pallas_call(
        functools.partial(dress_kernel, spin, pieces),
        out_shape=outs,
        in_specs=[SMEM, VMEM, ANY],
        out_specs=[VMEM] * len(outs),
        scratch_shapes=scratch,
        compiler_params=params(58),
        cost_estimate=pl.CostEstimate(
            flops=8 * order * order * sum(widths),
            bytes_accessed=8 * order * sum(widths),
            transcendentals=0,
        ),
        name="dress",
    )(where, phi, tile)
    flat = list(flat)
    return [[flat.pop(0) for _ in range(n)] for n in pieces]


def clear(sums_ref):
    def one(i, carry):
        sums_ref[i] = jnp.zeros(sums_ref.shape[1:], F32)
        return carry

    lax.fori_loop(0, sums_ref.shape[0], one, 0)


def add_slabs(dest_ref, sink, tile_ref, sums_ref, base=0):
    groups, slab_rows, _ = sums_ref.shape

    def one(b, carry):
        dest = dest_ref[sink, b] - base

        @pl.when(jnp.logical_and(dest >= 0, dest < groups))
        def _():
            start = pl.multiple_of(b * slab_rows, slab_rows)
            sums_ref[dest] += tile_ref[pl.ds(start, slab_rows), :].astype(F32)

        return carry

    lax.fori_loop(0, tile_ref.shape[0] // slab_rows, one, 0)


def gather_kernel(count, sinks_ref, dest_ref, *refs):
    sums_ref = refs[count]
    clear(sums_ref)
    for i, tile_ref in enumerate(refs[:count]):
        add_slabs(dest_ref, sinks_ref[i], tile_ref, sums_ref)


def gather(sinks, dest, tiles, groups):
    order, width = tiles[0].shape
    slab_rows = order // dest.shape[1]
    return pl.pallas_call(
        functools.partial(gather_kernel, len(tiles)),
        out_shape=jax.ShapeDtypeStruct((groups, slab_rows, width), F32),
        in_specs=[SMEM, SMEM] + [VMEM] * len(tiles),
        out_specs=VMEM,
        compiler_params=params(24),
        cost_estimate=pl.CostEstimate(
            flops=len(tiles) * order * width,
            bytes_accessed=2 * len(tiles) * order * width + 4 * groups * slab_rows * width,
            transcendentals=0,
        ),
        name="gather",
    )(sinks, dest, *tiles)


def finish_kernel(count, late, nodes, base, first, last, sinks_ref, dest_ref, here_ref, *refs):
    refs = list(refs)
    early_ref = None if late == count else refs.pop(0)
    before_ref = None if first else refs.pop(0)
    tiles = [refs.pop(0) for _ in range(count)]
    total_ref = refs.pop() if last else refs[0]
    left_ref = refs.pop()
    sums_ref = refs.pop()
    outs = refs
    order, width = tiles[0].shape
    half = width // 2
    slab_rows = sums_ref.shape[1]

    groups = sums_ref.shape[0]
    start = base * count
    if early_ref is None:
        clear(sums_ref)
    else:

        def take(i, carry):
            sums_ref[i] = early_ref[start + i]
            return carry

        lax.fori_loop(0, groups, take, 0, unroll=4)
    for i in range(count - late, count):
        add_slabs(dest_ref, sinks_ref[i], tiles[i], sums_ref, start)

    def place(node, carry):
        rows = pl.multiple_of(node * 2 * slab_rows, 2 * slab_rows)
        for i in range(count):
            real = sums_ref[node * count + i, :, :half].astype(BF16)
            imag = sums_ref[node * count + i, :, half:].astype(BF16)
            one = slice(i * width, i * width + half)
            two = slice(i * width + half, (i + 1) * width)
            left_ref[pl.ds(rows, slab_rows), one] = real
            left_ref[pl.ds(rows + slab_rows, slab_rows), one] = imag
            left_ref[pl.ds(rows, slab_rows), two] = imag
            left_ref[pl.ds(rows + slab_rows, slab_rows), two] = -real
        return carry

    lax.fori_loop(0, nodes, place, 0, unroll=True)
    block = 256

    def multiply(j, carry):
        cols = pl.ds(pl.multiple_of(j * block, block), block)
        rows = pl.ds(2 * base, 2 * nodes)
        product = 0.0 if first else before_ref[rows, :, cols].reshape(-1, block)
        for i in range(count):
            product += lax.dot_general(
                left_ref[:, i * width : (i + 1) * width],
                tiles[i][cols, :],
                (((1,), (1,)), ((), ())),
                preferred_element_type=F32,
            )
        total_ref[:, :, cols] = product.reshape(2 * nodes, slab_rows, block)
        return carry

    lax.fori_loop(0, order // block, multiply, 0, unroll=True)
    if last:
        rows = slab_rows // len(outs)
        for u, out_ref in enumerate(outs):
            start = pl.multiple_of((here_ref[0] ^ u) * rows, rows)
            out_ref[...] = total_ref[:, pl.ds(start, rows), :].astype(out_ref.dtype)


def finish(sinks, dest, here, sums, before, tiles, late, nodes, base, parts):
    order, width = tiles[0].shape
    count = len(tiles)
    slab_rows = order // dest.shape[1]
    first, last = before is None, parts > 0
    whole = jax.ShapeDtypeStruct((2 * nodes, slab_rows, order), F32)
    shape = (2 * nodes, slab_rows // max(parts, 1), order)
    outs = [jax.ShapeDtypeStruct(shape, BF16 if u else F32) for u in range(parts)]
    extra = [a for a in (sums, before) if a is not None]
    scratch = [
        pltpu.VMEM((count * nodes, slab_rows, width), F32),
        pltpu.VMEM((2 * nodes * slab_rows, count * width), BF16),
    ]
    if last:
        scratch.append(pltpu.VMEM(whole.shape, F32))
    return pl.pallas_call(
        functools.partial(finish_kernel, count, late, nodes, base, first, last),
        out_shape=outs if last else [whole],
        in_specs=[SMEM, SMEM, SMEM] + [VMEM] * (count + len(extra)),
        out_specs=[VMEM] * max(parts, 1),
        scratch_shapes=scratch,
        compiler_params=params(FINISH_MIB),
        cost_estimate=pl.CostEstimate(
            flops=8 * nodes * slab_rows * order * count * width,
            bytes_accessed=2 * count * order * width,
            transcendentals=0,
        ),
        name="finish",
    )(sinks, dest, here, *extra, *tiles)


def on_device(perambulator, elementals, momentum, routes, node_of, owner_slot):
    tile = perambulator[0, 0]
    order = tile.shape[1]
    eigen = elementals.shape[-1]
    spin = order // eigen
    sink_count = lax.axis_size("snk")
    source_count = lax.axis_size("src")
    chips = sink_count // 2
    width = order // chips
    node_count = owner_slot.shape[0]
    nodes = node_count // 2
    sink = lax.axis_index("snk")
    source = lax.axis_index("src")
    chip, core = sink // 2, sink % 2
    raw = chips // 2
    steps = [t for t in range(1, chips) if t != raw]
    sends = lambda value, t: swap(value, "snk", sink_count, 2 * t)
    column = lambda t: (chip ^ t).astype(jnp.int32).reshape(1)

    route = routes[0, :, :, 0]
    node_ids = jnp.arange(node_count, dtype=jnp.int32)
    match = (node_of[0][:, :, None] == node_ids).astype(jnp.int32)
    position = jnp.sum(match * owner_slot, axis=2)
    partner = 2 * ((route // 2) ^ chip) + ((route % 2) ^ core)

    chunks = 2 if width % 256 == 0 else 1
    part = width // chunks
    tie = lax.optimization_barrier

    piece = lax.dynamic_index_in_dim(elementals[0], momentum[0], 0, False)
    far_piece = sends(piece, raw)
    first = cut(tile, column(raw) * chunks, part)
    far_raw = sends(first, raw)
    phi = lax.all_gather(piece, "src", axis=1, tiled=True)
    far_phi = lax.all_gather(far_piece, "src", axis=1, tiled=True)
    own = {}
    next_t = steps[-1]
    (next_first,) = dress(phi, spin, tile, column(next_t) * chunks, [part], [1])[0]
    phi, next_first = tie((phi, next_first))
    rest = [(raw, 1), (next_t, 1)] if chunks > 1 else []
    rest += [(t, 0) for t in steps[-2::-1] + [0]]
    made = dress(
        phi,
        spin,
        tile,
        jnp.concatenate([column(t) * chunks + 1 if c else column(t) for t, c in rest]),
        [part if c else width for t, c in rest],
        [1 if c else chunks for t, c in rest],
    )
    for (t, c), arrays in zip(rest, made):
        own[t] = [None] * c + list(arrays)
    own.setdefault(next_t, [None])[0] = next_first

    here = source.astype(jnp.int32).reshape(1)
    arrival = [0, raw] + steps
    sinks = []
    places = []
    for t in arrival:
        sinks += [2 * (chip ^ t) + core, 2 * (chip ^ t) + (1 - core)]
        places += [2 * t, 2 * t + 1]
    sinks = jnp.stack(sinks).astype(jnp.int32)
    rank = jnp.array([places.index(i) for i in range(sink_count)], jnp.int32)
    ids = jnp.arange(sink_count, dtype=jnp.int32)
    order_of = jnp.sum((partner[:, :, None] == ids).astype(jnp.int32) * rank, axis=2)
    slot = ((position // 2) ^ chip) * sink_count + order_of
    dest = jnp.where(position % 2 == core, slot, -1).astype(jnp.int32)

    total = None
    seen = {}
    for c in range(chunks):
        here_now = {0: own[0][c]}
        if c:
            for t in [raw] + steps:
                sent, _ = tie((own[t][c], seen[t]))
                here_now[t] = sends(sent, t)
        else:
            for t in steps[::-1]:
                here_now[t] = seen[t] = sends(own[t][c], t)
            seen[raw] = far_raw
            for t in steps[:-1]:
                seen[t] = own[t][0]
            zero = jnp.zeros((1,), jnp.int32)
            (here_now[raw],) = dress(far_phi, spin, far_raw, zero, [part], [1])[0]
        tiles = []
        for t in arrival:
            tiles += [here_now[t], swap(here_now[t], "snk", sink_count, 1)]
        count = len(tiles)
        if c < chunks - 1:
            (total,) = finish(sinks, dest, here, None, total, tiles, count, nodes, 0, 0)
        else:
            late = 2
            sums = gather(sinks, dest, tiles[: count - late], sink_count * nodes)

    half = nodes // 2
    kept = []
    for base in (half, 0):
        outs = finish(sinks, dest, here, sums, total, tiles, late, half, base, source_count)
        moved = [outs[0]]
        for u in list(range(1, source_count))[::-1]:
            moved.append(swap(outs[u], "src", source_count, u).astype(F32))
        summed = functools.reduce(jnp.add, moved)
        summed = summed.reshape((half, 2) + summed.shape[1:])
        for t in list(range(base, base + half))[::-1]:
            value = summed[t - base]
            kept.append(sends(value.astype(BF16), t).astype(F32) if t else value)
    return functools.reduce(jnp.add, kept[::-1])[None]


def solution(mesh):
    placed = (
        P("src", "snk", None, None, None),
        P("snk", None, None, "src", None),
        P("snk"),
        P("src", None, None, None),
        P("src", None, None),
        P(),
    )
    return jax.shard_map(
        on_device,
        mesh=mesh,
        in_specs=placed,
        out_specs=P("snk", None, "src", None),
        check_vma=False,
    )
```

```python
import functools

import jax
import jax.numpy as jnp
from jax import lax
from jax.experimental import pallas as pl
from jax.experimental.pallas import tpu as pltpu
from jax.sharding import PartitionSpec as P


FINISH_MIB = 40
F32 = jnp.float32
BF16 = jnp.bfloat16
VMEM = pl.BlockSpec(memory_space=pltpu.VMEM)
SMEM = pl.BlockSpec(memory_space=pltpu.SMEM)
ANY = pl.BlockSpec(memory_space=pl.ANY)


def params(mib):
    return pltpu.CompilerParams(vmem_limit_bytes=mib * 1024 * 1024)


def swap(value, axis, size, flip):
    return lax.ppermute(value, axis, [(i, i ^ flip) for i in range(size)])


def cut_kernel(steps, where_ref, tile_hbm, out_hbm, held_ref, in_sems, out_sems):
    order, width = held_ref.shape
    half = width // 2
    start = pl.multiple_of(where_ref[0] * half, half)
    rows = order // steps
    into, out = [], []
    for i in range(steps):
        span = slice(i * rows, (i + 1) * rows)
        for x in range(2):
            held = held_ref.at[span, x * half : (x + 1) * half]
            into.append(
                pltpu.make_async_copy(
                    tile_hbm.at[x, span, pl.ds(start, half)], held, in_sems.at[2 * i + x]
                )
            )
            out.append(
                pltpu.make_async_copy(
                    held, out_hbm.at[span, x * half : (x + 1) * half], out_sems.at[2 * i + x]
                )
            )
    for copy in into:
        copy.start()
    for copy, onward in zip(into, out):
        copy.wait()
        onward.start()
    for onward in out:
        onward.wait()


def cut(tile, where, width):
    _, order, _ = tile.shape
    steps = 4
    return pl.pallas_call(
        functools.partial(cut_kernel, steps),
        out_shape=jax.ShapeDtypeStruct((order, 2 * width), tile.dtype),
        in_specs=[SMEM, ANY],
        out_specs=ANY,
        scratch_shapes=[
            pltpu.VMEM((order, 2 * width), tile.dtype),
            pltpu.SemaphoreType.DMA((2 * steps,)),
            pltpu.SemaphoreType.DMA((2 * steps,)),
        ],
        compiler_params=params(60),
        cost_estimate=pl.CostEstimate(
            flops=0, bytes_accessed=8 * order * width, transcendentals=0
        ),
        name="cut",
    )(where, tile)


def dress_kernel(spin, pieces, where_ref, phi_ref, tile_ref, *refs):
    refs = list(refs)
    outs = [[refs.pop(0) for _ in range(n)] for n in pieces]
    sems = refs.pop()
    wide_ref = refs.pop()
    rights = refs
    order = wide_ref.shape[0]
    eigen = order // spin
    copies = []
    for j, right_ref in enumerate(rights):
        width = right_ref.shape[1] // 2
        for x in range(2):
            if len(tile_ref.shape) == 3:
                start = pl.multiple_of(where_ref[j] * width, width)
                source = tile_ref.at[x, :, pl.ds(start, width)]
            else:
                source = tile_ref.at[:, x * width : (x + 1) * width]
            target = right_ref.at[:order, x * width : (x + 1) * width]
            copies.append(pltpu.make_async_copy(source, target, sems.at[2 * j + x]))
            copies[-1].start()

    row = lax.broadcasted_iota(jnp.int32, (order, eigen), 0)
    col = lax.broadcasted_iota(jnp.int32, (order, eigen), 1)
    spread = (row // spin == col).astype(BF16)
    r = lax.broadcasted_iota(jnp.int32, (eigen, order), 0)
    c = lax.broadcasted_iota(jnp.int32, (eigen, order), 1)
    same = r % spin == c % spin
    for x in range(2):
        tall = jnp.dot(spread, phi_ref[x], preferred_element_type=F32).astype(BF16)
        for part in range(spin):
            rows = slice(part * eigen, (part + 1) * eigen)
            wide = lax.dot_general(
                tall[rows], spread, (((1,), (1,)), ((), ())), preferred_element_type=F32
            )
            wide_ref[rows, x * order : (x + 1) * order] = jnp.where(same, wide, 0.0).astype(BF16)

    block = 256
    for j, right_ref in enumerate(rights):
        copies[2 * j].wait()
        copies[2 * j + 1].wait()
        width = right_ref.shape[1] // 2
        right_ref[order:, :width] = -right_ref[:order, width:]
        right_ref[order:, width:] = right_ref[:order, :width]

        def multiply(i, carry):
            rows = pl.ds(pl.multiple_of(i * block, block), block)
            both = jnp.dot(
                wide_ref[rows, :], right_ref[...], preferred_element_type=F32
            ).astype(BF16)
            part = width // len(outs[j])
            for k, out_ref in enumerate(outs[j]):
                out_ref[rows, :part] = both[:, k * part : (k + 1) * part]
                out_ref[rows, part:] = both[:, width + k * part : width + (k + 1) * part]
            return carry

        lax.fori_loop(0, order // block, multiply, 0)


def dress(phi, spin, tile, where, widths, pieces):
    order = phi.shape[-1] * spin
    outs = []
    for width, n in zip(widths, pieces):
        outs += [jax.ShapeDtypeStruct((order, 2 * width // n), BF16)] * n
    scratch = [pltpu.VMEM((2 * order, 2 * width), BF16) for width in widths]
    scratch += [
        pltpu.VMEM((order, 2 * order), BF16),
        pltpu.SemaphoreType.DMA((2 * len(widths),)),
    ]
    flat = pl.pallas_call(
        functools.partial(dress_kernel, spin, pieces),
        out_shape=outs,
        in_specs=[SMEM, VMEM, ANY],
        out_specs=[VMEM] * len(outs),
        scratch_shapes=scratch,
        compiler_params=params(58),
        cost_estimate=pl.CostEstimate(
            flops=8 * order * order * sum(widths),
            bytes_accessed=8 * order * sum(widths),
            transcendentals=0,
        ),
        name="dress",
    )(where, phi, tile)
    flat = list(flat)
    return [[flat.pop(0) for _ in range(n)] for n in pieces]


def clear(sums_ref):
    def one(i, carry):
        sums_ref[i] = jnp.zeros(sums_ref.shape[1:], F32)
        return carry

    lax.fori_loop(0, sums_ref.shape[0], one, 0)


def add_slabs(dest_ref, sink, tile_ref, sums_ref, base=0):
    groups, slab_rows, _ = sums_ref.shape

    def one(b, carry):
        dest = dest_ref[sink, b] - base

        @pl.when(jnp.logical_and(dest >= 0, dest < groups))
        def _():
            start = pl.multiple_of(b * slab_rows, slab_rows)
            sums_ref[dest] += tile_ref[pl.ds(start, slab_rows), :].astype(F32)

        return carry

    lax.fori_loop(0, tile_ref.shape[0] // slab_rows, one, 0, unroll=4)


def gather_kernel(count, more, sinks_ref, dest_ref, *refs):
    sums_ref = refs[-1]
    if more:

        def take(i, carry):
            sums_ref[i] = refs[count][i]
            return carry

        lax.fori_loop(0, sums_ref.shape[0], take, 0, unroll=4)
    else:
        clear(sums_ref)
    for i, tile_ref in enumerate(refs[:count]):
        add_slabs(dest_ref, sinks_ref[i], tile_ref, sums_ref)


def gather(sinks, dest, tiles, groups, before=None):
    more = [] if before is None else [before]
    order, width = tiles[0].shape
    slab_rows = order // dest.shape[1]
    return pl.pallas_call(
        functools.partial(gather_kernel, len(tiles), bool(more)),
        out_shape=jax.ShapeDtypeStruct((groups, slab_rows, width), F32),
        in_specs=[SMEM, SMEM] + [VMEM] * (len(tiles) + len(more)),
        out_specs=VMEM,
        compiler_params=params(24),
        cost_estimate=pl.CostEstimate(
            flops=len(tiles) * order * width,
            bytes_accessed=2 * len(tiles) * order * width + 4 * groups * slab_rows * width,
            transcendentals=0,
        ),
        name="gather",
    )(sinks, dest, *tiles, *more)


def finish_kernel(count, late, nodes, base, first, last, sinks_ref, dest_ref, here_ref, *refs):
    refs = list(refs)
    early_ref = None if late == count else refs.pop(0)
    before_ref = None if first else refs.pop(0)
    tiles = [refs.pop(0) for _ in range(count)]
    total_ref = refs.pop() if last else refs[0]
    left_ref = refs.pop()
    sums_ref = refs.pop()
    outs = refs
    order, width = tiles[0].shape
    half = width // 2
    slab_rows = sums_ref.shape[1]

    groups = sums_ref.shape[0]
    start = base * count
    if early_ref is None:
        clear(sums_ref)
    else:

        def take(i, carry):
            sums_ref[i] = early_ref[start + i]
            return carry

        lax.fori_loop(0, groups, take, 0, unroll=4)
    for i in range(count - late, count):
        add_slabs(dest_ref, sinks_ref[i], tiles[i], sums_ref, start)

    def place(node, carry):
        rows = pl.multiple_of(node * 2 * slab_rows, 2 * slab_rows)
        for i in range(count):
            real = sums_ref[node * count + i, :, :half].astype(BF16)
            imag = sums_ref[node * count + i, :, half:].astype(BF16)
            one = slice(i * width, i * width + half)
            two = slice(i * width + half, (i + 1) * width)
            left_ref[pl.ds(rows, slab_rows), one] = real
            left_ref[pl.ds(rows + slab_rows, slab_rows), one] = imag
            left_ref[pl.ds(rows, slab_rows), two] = imag
            left_ref[pl.ds(rows + slab_rows, slab_rows), two] = -real
        return carry

    lax.fori_loop(0, nodes, place, 0, unroll=True)
    block = 512

    def multiply(j, carry):
        cols = pl.ds(pl.multiple_of(j * block, block), block)
        rows = pl.ds(2 * base, 2 * nodes)
        product = 0.0 if first else before_ref[rows, :, cols].reshape(-1, block)
        for i in range(count):
            product += lax.dot_general(
                left_ref[:, i * width : (i + 1) * width],
                tiles[i][cols, :],
                (((1,), (1,)), ((), ())),
                preferred_element_type=F32,
            )
        total_ref[:, :, cols] = product.reshape(2 * nodes, slab_rows, block)
        return carry

    lax.fori_loop(0, order // block, multiply, 0, unroll=True)
    if last:
        rows = slab_rows // len(outs)
        for u, out_ref in enumerate(outs):
            start = pl.multiple_of((here_ref[0] ^ u) * rows, rows)
            out_ref[...] = total_ref[:, pl.ds(start, rows), :].astype(out_ref.dtype)


def finish(sinks, dest, here, sums, before, tiles, late, nodes, base, parts):
    order, width = tiles[0].shape
    count = len(tiles)
    slab_rows = order // dest.shape[1]
    first, last = before is None, parts > 0
    whole = jax.ShapeDtypeStruct((2 * nodes, slab_rows, order), F32)
    shape = (2 * nodes, slab_rows // max(parts, 1), order)
    outs = [jax.ShapeDtypeStruct(shape, BF16 if u else F32) for u in range(parts)]
    extra = [a for a in (sums, before) if a is not None]
    scratch = [
        pltpu.VMEM((count * nodes, slab_rows, width), F32),
        pltpu.VMEM((2 * nodes * slab_rows, count * width), BF16),
    ]
    if last:
        scratch.append(pltpu.VMEM(whole.shape, F32))
    return pl.pallas_call(
        functools.partial(finish_kernel, count, late, nodes, base, first, last),
        out_shape=outs if last else [whole],
        in_specs=[SMEM, SMEM, SMEM] + [VMEM] * (count + len(extra)),
        out_specs=[VMEM] * max(parts, 1),
        scratch_shapes=scratch,
        compiler_params=params(FINISH_MIB),
        cost_estimate=pl.CostEstimate(
            flops=8 * nodes * slab_rows * order * count * width,
            bytes_accessed=2 * count * order * width,
            transcendentals=0,
        ),
        name="finish",
    )(sinks, dest, here, *extra, *tiles)


def on_device(perambulator, elementals, momentum, routes, node_of, owner_slot):
    tile = perambulator[0, 0]
    order = tile.shape[1]
    eigen = elementals.shape[-1]
    spin = order // eigen
    sink_count = lax.axis_size("snk")
    source_count = lax.axis_size("src")
    chips = sink_count // 2
    width = order // chips
    node_count = owner_slot.shape[0]
    nodes = node_count // 2
    sink = lax.axis_index("snk")
    source = lax.axis_index("src")
    chip, core = sink // 2, sink % 2
    raw = chips // 2
    steps = [t for t in range(1, chips) if t != raw]
    sends = lambda value, t: swap(value, "snk", sink_count, 2 * t)
    column = lambda t: (chip ^ t).astype(jnp.int32).reshape(1)

    route = routes[0, :, :, 0]
    node_ids = jnp.arange(node_count, dtype=jnp.int32)
    match = (node_of[0][:, :, None] == node_ids).astype(jnp.int32)
    position = jnp.sum(match * owner_slot, axis=2)
    partner = 2 * ((route // 2) ^ chip) + ((route % 2) ^ core)

    chunks = 2 if width % 256 == 0 else 1
    part = width // chunks
    tie = lax.optimization_barrier

    piece = lax.dynamic_index_in_dim(elementals[0], momentum[0], 0, False)
    far_piece = sends(piece, raw)
    first = cut(tile, column(raw) * chunks, part)
    far_raw = sends(first, raw)
    phi = lax.all_gather(piece, "src", axis=1, tiled=True)
    far_phi = lax.all_gather(far_piece, "src", axis=1, tiled=True)
    own = {}
    next_t = steps[-1]
    (next_first,) = dress(phi, spin, tile, column(next_t) * chunks, [part], [1])[0]
    phi, next_first = tie((phi, next_first))
    rest = [(raw, 1), (next_t, 1)] if chunks > 1 else []
    rest += [(t, 0) for t in steps[-2::-1] + [0]]
    made = dress(
        phi,
        spin,
        tile,
        jnp.concatenate([column(t) * chunks + 1 if c else column(t) for t, c in rest]),
        [part if c else width for t, c in rest],
        [1 if c else chunks for t, c in rest],
    )
    for (t, c), arrays in zip(rest, made):
        own[t] = [None] * c + list(arrays)
    own.setdefault(next_t, [None])[0] = next_first

    here = source.astype(jnp.int32).reshape(1)
    arrival = [0, raw] + steps
    sinks = []
    places = []
    for t in arrival:
        sinks += [2 * (chip ^ t) + core, 2 * (chip ^ t) + (1 - core)]
        places += [2 * t, 2 * t + 1]
    sinks = jnp.stack(sinks).astype(jnp.int32)
    rank = jnp.array([places.index(i) for i in range(sink_count)], jnp.int32)
    ids = jnp.arange(sink_count, dtype=jnp.int32)
    order_of = jnp.sum((partner[:, :, None] == ids).astype(jnp.int32) * rank, axis=2)
    slot = ((position // 2) ^ chip) * sink_count + order_of
    dest = jnp.where(position % 2 == core, slot, -1).astype(jnp.int32)

    total = None
    seen = {}
    for c in range(chunks):
        here_now = {0: own[0][c]}
        if c:
            for t in [raw] + steps:
                sent, _ = tie((own[t][c], seen[t]))
                here_now[t] = sends(sent, t)
        else:
            for t in steps[::-1]:
                here_now[t] = seen[t] = sends(own[t][c], t)
            seen[raw] = far_raw
            for t in steps[:-1]:
                seen[t] = own[t][0]
            zero = jnp.zeros((1,), jnp.int32)
            (here_now[raw],) = dress(far_phi, spin, far_raw, zero, [part], [1])[0]
        tiles = []
        for t in arrival:
            tiles += [here_now[t], swap(here_now[t], "snk", sink_count, 1)]
        count = len(tiles)
        if c < chunks - 1:
            (total,) = finish(sinks, dest, here, None, total, tiles, count, nodes, 0, 0)
        else:
            late = 1
            sums = gather(sinks, dest, tiles[: count - 2], sink_count * nodes)
            sums = gather(sinks[count - 2 :], dest, tiles[-2:-1], sink_count * nodes, sums)

    half = nodes // 2
    kept = []
    for base in (half, 0):
        outs = finish(sinks, dest, here, sums, total, tiles, late, half, base, source_count)
        moved = [outs[0]]
        for u in list(range(1, source_count))[::-1]:
            moved.append(swap(outs[u], "src", source_count, u).astype(F32))
        summed = functools.reduce(jnp.add, moved)
        summed = summed.reshape((half, 2) + summed.shape[1:])
        for t in range(base, base + half):
            value = summed[t - base]
            kept.append(sends(value.astype(BF16), t).astype(F32) if t else value)
    return functools.reduce(jnp.add, kept[::-1])[None]


def solution(mesh):
    placed = (
        P("src", "snk", None, None, None),
        P("snk", None, None, "src", None),
        P("snk"),
        P("src", None, None, None),
        P("src", None, None),
        P(),
    )
    return jax.shard_map(
        on_device,
        mesh=mesh,
        in_specs=placed,
        out_specs=P("snk", None, "src", None),
        check_vma=False,
    )
```
